128 devices in a mesh: band: 8 (over x, y_lo), slab: 16 (over z, y_hi, core).
Axes of the slice: x: 4, y: 4 (y_hi: 2, y_lo: 2; y = y_hi * 2 + y_lo), z: 4, core: 2. Of those that a mesh axis runs over, the one named last changes fastest.
Arguments:
- band_fields: float32 [16, 6, 6, 128, 2048], P(None, None, None, ('band', 'slab')), may hold values from -12 to 12
Outputs:
- pair_transfer: float32 [16, 16, 2048], P('band', None, 'slab')
The draws below stay inside these ranges and needn't reach their ends.
All inputs are finite; a program needn't handle non-finite values.
Results may differ from the reference program's by a relative error of at most 0.0042.
Values may be sent and summed in bfloat16 or wider, within the bound.
A program may use at most 192 MiB of HBM per device.

```python
import jax
import jax.numpy as jnp
from jax import lax

NBANDS = 16
XW = 4
NY = 128
XIN = 6
NZ = 2048


def block_scale(key, dims, cuts, least, largest):
    gain, own = 1.0, jax.random.fold_in(key, 6)
    for position, blocks in cuts:
        draws = jnp.exp(jax.random.uniform(jax.random.fold_in(own, position), (blocks,), jnp.float32, least / len(cuts), largest / len(cuts)))
        gain = gain * jnp.repeat(draws, dims[position] // blocks).reshape([-1 if axis == position else 1 for axis in range(len(dims))])
    return gain


def gaussian(own_key, shape, width, most, pieces=(), held_as=jnp.bfloat16):
    array = width * jax.random.normal(own_key, shape, jnp.float32)
    if pieces:
        array = array * block_scale(own_key, shape, pieces, -0.22, 0.18)
    return jnp.clip(array, -most, most).astype(held_as)


def setup_inputs(seed: int = 0) -> dict:
    key_list = jax.random.split(jax.random.key(seed), 2)
    return {
        "band_fields": gaussian(key_list[0], (NBANDS, 6, XIN, NY, NZ), 2.0, 12.0, ((3, 128),), jnp.float32),
    }


hall_length = 0.5


def derivs(field):
    inner = field[:, 1:-1]
    ddx = (field[:, 2:] - field[:, :-2]) * 0.5
    ddy = (jnp.roll(inner, -1, 2) - jnp.roll(inner, 1, 2)) * 0.5
    ddz = (jnp.roll(inner, -1, 3) - jnp.roll(inner, 1, 3)) * 0.5
    return inner, ddx, ddy, ddz


def curl_of(ddx, ddy, ddz):
    return jnp.stack([ddy[5] - ddz[4], ddz[3] - ddx[5], ddx[4] - ddy[3]])


def advect(vector, ddx, ddy, ddz, first):
    return vector[0] * ddx[first:first + 3] + vector[1] * ddy[first:first + 3] + vector[2] * ddz[first:first + 3]


def drive_of(inner, ddx, ddy, ddz, velocity, magnetic, current):
    part_a = -advect(velocity, ddx, ddy, ddz, 0) + advect(magnetic, ddx, ddy, ddz, 3)
    part_c = -advect(velocity, ddx, ddy, ddz, 3) + advect(magnetic, ddx, ddy, ddz, 0)
    bfield = inner[3:6]
    cross = jnp.stack([current[1] * bfield[2] - current[2] * bfield[1], current[2] * bfield[0] - current[0] * bfield[2], current[0] * bfield[1] - current[1] * bfield[0]])
    return jnp.concatenate([part_a, part_c, -hall_length * cross], 0)


def reference(band_fields):
    def sums_of(field):
        inner, ddx, ddy, ddz = derivs(field)
        return jnp.concatenate([inner, curl_of(ddx, ddy, ddz)], 0)

    responses = lax.map(sums_of, band_fields)
    full = jnp.sum(responses, 0)
    velocity, magnetic, current = full[0:3], full[3:6], full[6:9]

    def drives_of(field):
        inner, ddx, ddy, ddz = derivs(field)
        return drive_of(inner, ddx, ddy, ddz, velocity, magnetic, current).astype(jnp.bfloat16)

    drives = lax.map(drives_of, band_fields)
    resp = responses.astype(jnp.bfloat16).astype(jnp.float32)
    total = jnp.einsum("qcxyz,kcxyz->qkz", resp, drives.astype(jnp.float32))
    return total * (1.0 / (XW * NY))
```

```python
import functools

import jax
import jax.numpy as jnp
from jax import lax
from jax.experimental import pallas as pl
from jax.experimental.pallas import tpu as pltpu
from jax.sharding import PartitionSpec as P

MESH = pl.DeviceIdType.MESH
F32 = jnp.float32
BF16 = jnp.bfloat16

STARTS = (0, 6, 12, 19, 25, 31)
SIZES = (6, 6, 7, 6, 6, 6)
EDGE = 18
TILES = 37


def kernel(nb, ns, x_ref, o_ref, xv, edges, send, recv, resp, drive, acc, parts,
           load_sem, own_sem, send_sem, recv_sem, hs_sem, hr_sem, ps_sem, pr_sem):
    band = lax.axis_index("band")
    slab = lax.axis_index("slab")

    load = pltpu.make_async_copy(x_ref, xv, load_sem)
    load.start()

    barrier = pltpu.get_barrier_semaphore()

    def greet_slab(k, carry):
        pl.semaphore_signal(barrier, inc=1, device_id=(band, lax.rem(slab + k, ns)), device_id_type=MESH)
        return carry

    def greet_band(k, carry):
        pl.semaphore_signal(barrier, inc=1, device_id=(lax.rem(band + k, nb), slab), device_id_type=MESH)
        return carry

    lax.fori_loop(1, ns, greet_slab, 0)
    lax.fori_loop(1, nb, greet_band, 0)
    load.wait()

    lane = lax.broadcasted_iota(jnp.int32, (16, 128), 1)
    pair = lane // 2

    def pack(s, carry):
        edge = jnp.zeros((16, 128), F32)
        for x in range(6):
            for c in range(6):
                tile = xv[pl.ds(c * 96 + x * 16 + s, 16, stride=576), :]
                send[s, STARTS[x] + c + (0), :, :] = tile.astype(BF16)
                if 1 <= x <= 4:
                    i = (x - 1) * 6 + c
                    edge = jnp.where(pair == i, pltpu.roll(tile, 2 * i + 1, 1), edge)
        edges[s] = edge
        return carry

    lax.fori_loop(0, ns, pack, 0)

    def pack_edges(s, carry):
        above = pltpu.roll(edges[lax.rem(s + 1, ns)], 127, 1)
        below = pltpu.roll(edges[lax.rem(s + ns - 1, ns)], 1, 1)
        send[s, EDGE] = jnp.where(lane - 2 * pair == 0, above, below).astype(BF16)
        return carry

    lax.fori_loop(0, ns, pack_edges, 0)

    own = pltpu.make_async_copy(send.at[slab], recv.at[slab + 1], own_sem)
    own.start()

    pl.semaphore_wait(barrier, ns - 1 + nb - 1)

    def message(x, k):
        to = lax.rem(slab + k, ns)
        tiles = pl.ds(STARTS[x], SIZES[x])
        return pltpu.make_async_remote_copy(
            src_ref=send.at[to, tiles],
            dst_ref=recv.at[slab + 1, tiles],
            send_sem=send_sem.at[x, k],
            recv_sem=recv_sem.at[x, k],
            device_id=(band, to),
            device_id_type=MESH,
        )

    for x in range(6):
        def start(k, carry, x=x):
            message(x, k).start()
            return carry
        lax.fori_loop(1, ns, start, 0)

    def wait_plane(x):
        def wait(k, carry):
            message(x, k).wait_recv()
            return carry
        lax.fori_loop(1, ns, wait, 0)

    def halo(x, up):
        tiles = pl.ds(STARTS[x], 6)
        return pltpu.make_async_remote_copy(
            src_ref=recv.at[ns if up else 1, tiles],
            dst_ref=recv.at[0 if up else ns + 1, tiles],
            send_sem=hs_sem.at[x - 1, up],
            recv_sem=hr_sem.at[x - 1, up],
            device_id=(lax.rem(band + (1 if up else nb - 1), nb), slab),
            device_id_type=MESH,
        )

    def compute(x):
        lo, mid, hi = STARTS[x - 1], STARTS[x], STARTS[x + 1]

        def fields(y, carry):
            def tile(row, t):
                return recv[row, t].astype(F32)

            edge = tile(y + 1, EDGE)
            inner, dx, dy, dz = [], [], [], []
            for c in range(6):
                value = tile(y + 1, mid + c)
                inner.append(value)
                dx.append(tile(y + 1, hi + c) - tile(y + 1, lo + c))
                dy.append(tile(y + 2, mid + c) - tile(y, mid + c))
                ends = pltpu.roll(edge, 127 - 2 * ((x - 1) * 6 + c), 1)
                upper = jnp.where(lane == 127, ends, pltpu.roll(value, 127, 1))
                lower = jnp.where(lane == 0, ends, pltpu.roll(value, 1, 1))
                dz.append(upper - lower)
            current = [dy[5] - dz[4], dz[3] - dx[5], dx[4] - dy[3]]

            def total(value, scale):
                return jnp.sum(value, axis=0, keepdims=True) * scale

            v = [total(inner[c], -0.5) for c in range(3)]
            b = [total(inner[3 + c], 0.5) for c in range(3)]
            j = [total(current[c], -0.25) for c in range(3)]
            for c in range(6):
                resp[y, c] = inner[c]
            for c in range(3):
                resp[y, 6 + c] = current[c] * 0.5
            for c in range(3):
                e = 3 + c
                drive[y, c] = (v[0] * dx[c] + v[1] * dy[c] + v[2] * dz[c]) + (
                    b[0] * dx[e] + b[1] * dy[e] + b[2] * dz[e])
                drive[y, e] = (v[0] * dx[e] + v[1] * dy[e] + v[2] * dz[e]) + (
                    b[0] * dx[c] + b[1] * dy[c] + b[2] * dz[c])
            drive[y, 6] = j[1] * inner[5] - j[2] * inner[4]
            drive[y, 7] = j[2] * inner[3] - j[0] * inner[5]
            drive[y, 8] = j[0] * inner[4] - j[1] * inner[3]
            return carry

        lax.fori_loop(0, ns, fields, 0)

        def contract(y, sums):
            sums = list(sums)
            for c in range(9):
                d = drive[y, c]
                for q in range(16):
                    sums[q] = sums[q] + resp[y, c, pl.ds(q, 1), :] * d
            return tuple(sums)

        if x == 1:
            first = tuple(jnp.zeros((16, 128), F32) for q in range(16))
        else:
            first = tuple(acc[q] for q in range(16))
        sums = lax.fori_loop(0, ns, contract, first)
        for q in range(16):
            acc[q] = sums[q]

    own.wait()
    wait_plane(0)
    for x in range(1, 6):
        wait_plane(x)
        if x <= 4:
            halo(x, 0).start()
            halo(x, 1).start()
        if x >= 2:
            halo(x - 1, 0).wait_recv()
            halo(x - 1, 1).wait_recv()
            compute(x - 1)

    def part(k):
        to = lax.rem(band + k, nb)
        return pltpu.make_async_remote_copy(
            src_ref=acc.at[pl.ds(2 * to, 2)],
            dst_ref=parts.at[k - 1],
            send_sem=ps_sem.at[k - 1],
            recv_sem=pr_sem.at[k - 1],
            device_id=(to, slab),
            device_id_type=MESH,
        )

    for k in range(1, nb):
        part(k).start()
    result = acc[pl.ds(2 * band, 2)]
    for k in range(1, nb):
        part(k).wait_recv()
        result = result + parts[k - 1]
    o_ref[...] = result * (1.0 / 512.0)

    for x in range(6):
        def drain(k, carry, x=x):
            message(x, k).wait_send()
            return carry
        lax.fori_loop(1, ns, drain, 0)
    for x in range(1, 5):
        halo(x, 0).wait_send()
        halo(x, 1).wait_send()
    for k in range(1, nb):
        part(k).wait_send()


def body(band_fields):
    nb, ns = lax.axis_size("band"), lax.axis_size("slab")
    rows = band_fields.reshape(16 * 36 * 16, 128)
    dma = pltpu.SemaphoreType.DMA
    return pl.pallas_call(
        functools.partial(kernel, nb, ns),
        out_shape=jax.ShapeDtypeStruct((2, 16, 128), F32),
        in_specs=[pl.BlockSpec(memory_space=pltpu.HBM)],
        out_specs=pl.BlockSpec(memory_space=pltpu.VMEM),
        scratch_shapes=[
            pltpu.VMEM((9216, 128), F32),
            pltpu.VMEM((ns, 16, 128), F32),
            pltpu.VMEM((ns, TILES, 16, 128), BF16),
            pltpu.VMEM((ns + 2, TILES, 16, 128), BF16),
            pltpu.VMEM((ns, 9, 16, 128), F32),
            pltpu.VMEM((ns, 9, 16, 128), F32),
            pltpu.VMEM((16, 16, 128), F32),
            pltpu.VMEM((nb - 1, 2, 16, 128), F32),
            dma,
            dma,
            dma((6, ns)),
            dma((6, ns)),
            dma((4, 2)),
            dma((4, 2)),
            dma((nb - 1,)),
            dma((nb - 1,)),
        ],
        compiler_params=pltpu.CompilerParams(
            collective_id=0, has_side_effects=True, vmem_limit_bytes=48 << 20
        ),
    )(rows)


def solution(mesh):
    return jax.shard_map(
        body,
        mesh=mesh,
        in_specs=(P(None, None, None, ("band", "slab"), None),),
        out_specs=P("band", None, "slab"),
        check_vma=False,
    )
```

```python
import functools

import jax
import jax.numpy as jnp
from jax import lax
from jax.experimental import pallas as pl
from jax.experimental.pallas import tpu as pltpu
from jax.sharding import PartitionSpec as P

MESH = pl.DeviceIdType.MESH
F32 = jnp.float32
BF16 = jnp.bfloat16

STARTS = (25, 0, 6, 12, 19, 31)
SIZES = (6, 6, 6, 7, 6, 6)
EDGE = 18
TILES = 37


def kernel(nb, ns, x_ref, o_ref, xv, edges, send, recv, resp, drive, acc, parts,
           load_sem, own_sem, send_sem, recv_sem, hs_sem, hr_sem, ps_sem, pr_sem):
    band = lax.axis_index("band")
    slab = lax.axis_index("slab")

    def load(x):
        return pltpu.make_async_copy(x_ref.at[:, x], xv.at[x], load_sem.at[x])

    barrier = pltpu.get_barrier_semaphore()

    def greet_slab(k, carry):
        pl.semaphore_signal(barrier, inc=1, device_id=(band, lax.rem(slab + k, ns)), device_id_type=MESH)
        return carry

    def greet_band(k, carry):
        pl.semaphore_signal(barrier, inc=1, device_id=(lax.rem(band + k, nb), slab), device_id_type=MESH)
        return carry

    lax.fori_loop(1, ns, greet_slab, 0)
    lax.fori_loop(1, nb, greet_band, 0)
    for x in range(6):
        load(x).start()

    lane = lax.broadcasted_iota(jnp.int32, (16, 128), 1)
    pair = lane // 2
    rows = xv.reshape(6 * 96 * 16, 128)

    def pack(x):
        load(x).wait()

        def step(s, carry):
            if 1 <= x <= 4:
                edge = jnp.zeros((16, 128), F32) if x == 1 else edges[s]
            for c in range(6):
                tile = rows[pl.ds(x * 1536 + c * 16 + s, 16, stride=96), :]
                send[s, STARTS[x] + c] = tile.astype(BF16)
                if 1 <= x <= 4:
                    i = (x - 1) * 6 + c
                    edge = jnp.where(pair == i, pltpu.roll(tile, 2 * i + 1, 1), edge)
            if 1 <= x <= 4:
                edges[s] = edge
            return carry

        lax.fori_loop(0, ns, step, 0)

    def pack_edges(s, carry):
        above = pltpu.roll(edges[lax.rem(s + 1, ns)], 127, 1)
        below = pltpu.roll(edges[lax.rem(s + ns - 1, ns)], 1, 1)
        send[s, EDGE] = jnp.where(lane - 2 * pair == 0, above, below).astype(BF16)
        return carry

    own = pltpu.make_async_copy(send.at[slab], recv.at[slab + 1], own_sem)

    def message(x, k):
        to = lax.rem(slab + k, ns)
        tiles = pl.ds(STARTS[x], SIZES[x])
        return pltpu.make_async_remote_copy(
            src_ref=send.at[to, tiles],
            dst_ref=recv.at[slab + 1, tiles],
            send_sem=send_sem.at[x, k],
            recv_sem=recv_sem.at[x, k],
            device_id=(band, to),
            device_id_type=MESH,
        )

    def start_plane(x):
        def start(k, carry):
            message(x, k).start()
            return carry
        lax.fori_loop(1, ns, start, 0)

    def drain_plane(x):
        def drain(k, carry):
            message(x, k).wait_send()
            return carry
        lax.fori_loop(1, ns, drain, 0)

    def wait_plane(x):
        def wait(k, carry):
            message(x, k).wait_recv()
            return carry
        lax.fori_loop(1, ns, wait, 0)

    def halo(x, up):
        tiles = pl.ds(STARTS[x], 6)
        return pltpu.make_async_remote_copy(
            src_ref=recv.at[ns if up else 1, tiles],
            dst_ref=recv.at[0 if up else ns + 1, tiles],
            send_sem=hs_sem.at[x - 1, up],
            recv_sem=hr_sem.at[x - 1, up],
            device_id=(lax.rem(band + (1 if up else nb - 1), nb), slab),
            device_id_type=MESH,
        )

    def compute(x):
        lo, mid, hi = STARTS[x - 1], STARTS[x], STARTS[x + 1]

        def fields(y, carry):
            def tile(row, t):
                return recv[row, t].astype(F32)

            edge = tile(y + 1, EDGE)
            inner, dx, dy, dz = [], [], [], []
            for c in range(6):
                value = tile(y + 1, mid + c)
                inner.append(value)
                dx.append(tile(y + 1, hi + c) - tile(y + 1, lo + c))
                dy.append(tile(y + 2, mid + c) - tile(y, mid + c))
                ends = pltpu.roll(edge, 127 - 2 * ((x - 1) * 6 + c), 1)
                upper = jnp.where(lane == 127, ends, pltpu.roll(value, 127, 1))
                lower = jnp.where(lane == 0, ends, pltpu.roll(value, 1, 1))
                dz.append(upper - lower)
            current = [dy[5] - dz[4], dz[3] - dx[5], dx[4] - dy[3]]

            def total(value, scale):
                return jnp.sum(value, axis=0, keepdims=True) * scale

            v = [total(inner[c], -0.5) for c in range(3)]
            b = [total(inner[3 + c], 0.5) for c in range(3)]
            j = [total(current[c], -0.25) for c in range(3)]
            for c in range(6):
                resp[y, c] = inner[c]
            for c in range(3):
                resp[y, 6 + c] = current[c] * 0.5
            for c in range(3):
                e = 3 + c
                drive[y, c] = (v[0] * dx[c] + v[1] * dy[c] + v[2] * dz[c]) + (
                    b[0] * dx[e] + b[1] * dy[e] + b[2] * dz[e])
                drive[y, e] = (v[0] * dx[e] + v[1] * dy[e] + v[2] * dz[e]) + (
                    b[0] * dx[c] + b[1] * dy[c] + b[2] * dz[c])
            drive[y, 6] = j[1] * inner[5] - j[2] * inner[4]
            drive[y, 7] = j[2] * inner[3] - j[0] * inner[5]
            drive[y, 8] = j[0] * inner[4] - j[1] * inner[3]
            return carry

        lax.fori_loop(1, ns - 1, fields, 0)
        halo(x, 0).wait_recv()
        halo(x, 1).wait_recv()
        lax.fori_loop(0, 2, lambda i, carry: fields(i * (ns - 1), carry), 0)

        def contract(y, sums):
            sums = list(sums)
            for c in range(9):
                d = drive[y, c]
                for q in range(16):
                    sums[q] = sums[q] + resp[y, c, pl.ds(q, 1), :] * d
            return tuple(sums)

        if x == 4:
            return
        if x == 2:
            first = tuple(jnp.zeros((16, 128), F32) for q in range(16))
        else:
            first = tuple(acc[q] for q in range(16))
        sums = lax.fori_loop(0, ns, contract, first)
        for q in range(16):
            acc[q] = sums[q]

    def part(k):
        to = lax.rem(band + k, nb)
        return pltpu.make_async_remote_copy(
            src_ref=acc.at[pl.ds(2 * to, 2)],
            dst_ref=parts.at[k - 1],
            send_sem=ps_sem.at[k - 1],
            recv_sem=pr_sem.at[k - 1],
            device_id=(to, slab),
            device_id_type=MESH,
        )

    def finish(steps):
        groups = [2 * lax.rem(band + k, nb) + r for k in steps for r in range(2)]

        def contract(y, sums):
            sums = list(sums)
            for c in range(9):
                d = drive[y, c]
                for i, q in enumerate(groups):
                    sums[i] = sums[i] + resp[y, c, pl.ds(q, 1), :] * d
            return tuple(sums)

        sums = lax.fori_loop(0, ns, contract, tuple(acc[q] for q in groups))
        for i, q in enumerate(groups):
            acc[q] = sums[i]
        for k in steps:
            if k:
                part(k).start()

    pack(1)
    pack(2)
    pl.semaphore_wait(barrier, ns - 1 + nb - 1)
    start_plane(1)
    start_plane(2)
    for x in (3, 4, 0, 5):
        pack(x)
    lax.fori_loop(0, ns, pack_edges, 0)
    own.start()
    drain_plane(1)
    start_plane(3)
    drain_plane(2)
    start_plane(4)
    own.wait()

    def arrive(x):
        wait_plane(x)
        if 1 <= x <= 4:
            halo(x, 0).start()
            halo(x, 1).start()

    arrive(1)
    arrive(2)
    arrive(3)
    drain_plane(3)
    start_plane(0)
    compute(2)
    arrive(4)
    drain_plane(4)
    start_plane(5)
    compute(3)
    arrive(0)
    compute(1)
    arrive(5)
    compute(4)
    for steps in ((4, 5), (3, 2), (6, 7), (1, 0)):
        finish(steps)

    result = acc[pl.ds(2 * band, 2)]
    for k in range(1, nb):
        part(k).wait_recv()
        result = result + parts[k - 1]
    o_ref[...] = result * (1.0 / 512.0)

    for x in (0, 5):
        drain_plane(x)
    for x in range(1, 5):
        halo(x, 0).wait_send()
        halo(x, 1).wait_send()
    for k in range(1, nb):
        part(k).wait_send()


def body(band_fields):
    nb, ns = lax.axis_size("band"), lax.axis_size("slab")
    rows = band_fields.reshape(96, 6, 16, 128)
    dma = pltpu.SemaphoreType.DMA
    return pl.pallas_call(
        functools.partial(kernel, nb, ns),
        out_shape=jax.ShapeDtypeStruct((2, 16, 128), F32),
        in_specs=[pl.BlockSpec(memory_space=pltpu.HBM)],
        out_specs=pl.BlockSpec(memory_space=pltpu.VMEM),
        scratch_shapes=[
            pltpu.VMEM((6, 96, 16, 128), F32),
            pltpu.VMEM((ns, 16, 128), F32),
            pltpu.VMEM((ns, TILES, 16, 128), BF16),
            pltpu.VMEM((ns + 2, TILES, 16, 128), BF16),
            pltpu.VMEM((ns, 9, 16, 128), F32),
            pltpu.VMEM((ns, 9, 16, 128), F32),
            pltpu.VMEM((16, 16, 128), F32),
            pltpu.VMEM((nb - 1, 2, 16, 128), F32),
            dma((6,)),
            dma,
            dma((6, ns)),
            dma((6, ns)),
            dma((4, 2)),
            dma((4, 2)),
            dma((nb - 1,)),
            dma((nb - 1,)),
        ],
        compiler_params=pltpu.CompilerParams(
            collective_id=0, has_side_effects=True, vmem_limit_bytes=62 << 20
        ),
    )(rows)


def solution(mesh):
    return jax.shard_map(
        body,
        mesh=mesh,
        in_specs=(P(None, None, None, ("band", "slab"), None),),
        out_specs=P("band", None, "slab"),
        check_vma=False,
    )
```
